32 devices in a mesh: grp: 4 (over z), tp: 4 (over y, x), rep: 2 (over core).
Axes of the slice: x: 2, y: 2, z: 4, core: 2. Of those that a mesh axis runs over, the one named last changes fastest.
Arguments:
- query_rows: bfloat16 [4, 1024, 2048], P('tp', ('grp', 'rep')), may hold values from -120 to 120
- key_rows: bfloat16 [4, 1024, 512], P('tp', ('grp', 'rep')), may hold values from -6 to 6, as said below
- value_rows: bfloat16 [4, 1024, 512], P('tp', ('grp', 'rep')), may hold values from -6 to 6
- teacher_codes: bfloat16 [4, 1024, 4096], P(None, ('grp', 'rep'), 'tp'), may hold values from -6 to 6
- teacher_scales: bfloat16 [4, 1024, 32], P(None, ('grp', 'rep'), 'tp'), may hold values from 0.099609375 to 1
- projection: bfloat16 [2048, 4096], P(None, ('grp', 'rep')), may hold values from -0.125 to 0.125
Outputs:
- grad_query: bfloat16 [4, 1024, 2048], P('tp', ('grp', 'rep'))
- grad_key: bfloat16 [4, 1024, 512], P('tp', ('grp', 'rep'))
- grad_value: bfloat16 [4, 1024, 512], P('tp', ('grp', 'rep'))
The draws below stay inside these ranges and needn't reach their ends.
Inputs may be any that keep to these rules, and one draw needn't show every extreme that they name: `key_rows`: keys of every head.
All inputs are finite; a program needn't handle non-finite values.
Results may differ from the reference program's by a relative error of at most 0.014.
Values may be sent and summed in bfloat16 or wider, within the bound.
A program may use at most 128 MiB of HBM per device.

```python
import math
import jax
import jax.numpy as jnp
from jax import lax

TOK_DEV = 128
HEADS = 16
KV_HEADS = 4
HEAD_DIM = 128
COLS = 4096
QBLOCK = 128
SEQS = 4
SEQ_LEN = 1024
N_GRP = 4
N_REP = 2


def paired_fields(key):
    query_noise = jax.random.normal(jax.random.fold_in(key, 101), (SEQS, SEQ_LEN, HEADS, HEAD_DIM), jnp.float32)
    key_noise = jax.random.normal(jax.random.fold_in(key, 202), (SEQS, SEQ_LEN, KV_HEADS, HEAD_DIM), jnp.float32)
    keys_field = jnp.clip(key_noise, -6.0, 6.0)
    queries_field = jnp.clip(2.0 * query_noise, -12.0, 12.0)
    queries_field = queries_field.reshape(SEQS, SEQ_LEN, HEADS * HEAD_DIM)
    keys_field = keys_field.reshape(SEQS, SEQ_LEN, KV_HEADS * HEAD_DIM)
    return (queries_field, keys_field)


def draw_query_rows(key, part):
    return paired_fields(key)[0].astype(jnp.bfloat16)


def draw_key_rows(key, part):
    return paired_fields(key)[1].astype(jnp.bfloat16)


def block_levels(stream_key, dims, shards, least, top_value):
    gain, own = 1.0, jax.random.fold_in(stream_key, 6)
    for axis_at, parts in shards:
        draws = jnp.exp(jax.random.uniform(jax.random.fold_in(own, axis_at), (parts,), jnp.float32, least / len(shards), top_value / len(shards)))
        gain = gain * jnp.repeat(draws, dims[axis_at] // parts).reshape([-1 if axis == axis_at else 1 for axis in range(len(dims))])
    return gain


def bell_draw(own_key, dims, width, reach, shards=(), kind=jnp.bfloat16):
    array = width * jax.random.normal(own_key, dims, jnp.float32)
    if shards:
        array = array * block_levels(own_key, dims, shards, -0.22, 0.18)
    return jnp.clip(array, -reach, reach).astype(kind)


def setup_inputs(seed: int = 0) -> dict:
    splits = jax.random.split(jax.random.key(seed), 7)
    return {
        "query_rows": draw_query_rows(jax.random.fold_in(splits[6], 71), 0),
        "key_rows": draw_key_rows(jax.random.fold_in(splits[6], 71), 0),
        "value_rows": bell_draw(splits[2], (SEQS, SEQ_LEN, KV_HEADS * HEAD_DIM), 1.0, 6.0, ((0, 4), (1, 8))),
        "teacher_codes": bell_draw(splits[3], (SEQS, SEQ_LEN, COLS), 1.0, 6.0, ((1, 8), (2, 4))),
        "teacher_scales": jnp.clip(jnp.exp(math.log(1.0) - 2.306499 * jax.random.uniform(splits[4], (SEQS, SEQ_LEN, COLS // QBLOCK), jnp.float32) ** block_levels(splits[4], (SEQS, SEQ_LEN, COLS // QBLOCK), ((1, 8), (2, 4)), -0.2, 0.2)), 0.099609375, 1.0).astype(jnp.bfloat16),
        "projection": bell_draw(splits[5], (HEADS * HEAD_DIM, COLS), (HEADS * HEAD_DIM) ** -0.5, 0.125, ((1, 8),)),
    }


masked_low = -1e+30

def reference(query_rows, key_rows, value_rows, teacher_codes, teacher_scales, projection):
    group_size = HEADS // KV_HEADS
    part_count = N_GRP * N_REP
    col_width = COLS // part_count
    block_count = SEQ_LEN // TOK_DEV
    inv_root = 1.0 / math.sqrt(HEAD_DIM)
    row_ids = jnp.arange(TOK_DEV, dtype=jnp.int32)
    col_ids = jnp.arange(SEQ_LEN, dtype=jnp.int32)
    highest = lax.Precision.HIGHEST

    def one_slab(slab_data):
        slab_query, slab_key, slab_value, slab_codes, slab_scales = slab_data
        key_heads = slab_key.reshape(SEQ_LEN, KV_HEADS, HEAD_DIM).transpose(1, 0, 2).astype(jnp.float32)
        value_heads = slab_value.reshape(SEQ_LEN, KV_HEADS, HEAD_DIM).transpose(1, 0, 2).astype(jnp.float32)

        def scan_step(running, block_index):
            grad_keys, grad_values = running
            first = (block_index * TOK_DEV).astype(jnp.int32)
            query_part = lax.dynamic_slice_in_dim(slab_query, first, TOK_DEV, 0)
            queries = query_part.reshape(TOK_DEV, KV_HEADS, group_size, HEAD_DIM).transpose(1, 2, 0, 3).astype(jnp.float32)
            raw_scores = jnp.einsum('hgqd,hkd->hgqk', queries, key_heads, precision=highest) * inv_root
            allowed = col_ids[None, :] <= (first + row_ids)[:, None]
            scores = jnp.where(allowed, raw_scores, masked_low)
            row_peak = scores.max(-1)
            shifted = jnp.exp(scores - row_peak[..., None])
            row_total = shifted.sum(-1)
            probs = shifted / row_total[..., None]
            prob_low = probs.astype(jnp.bfloat16)
            attn_wide = jnp.einsum('hgqk,hkd->hgqd', prob_low.astype(jnp.float32), value_heads, precision=highest)
            attn_flat = attn_wide.transpose(2, 0, 1, 3).reshape(TOK_DEV, HEADS * HEAD_DIM)
            attn_low = attn_flat.astype(jnp.bfloat16)
            approx = jnp.dot(attn_low, projection, preferred_element_type=jnp.float32)
            code_rows = lax.dynamic_slice_in_dim(slab_codes, first, TOK_DEV, 0).astype(jnp.float32)
            scale_rows = lax.dynamic_slice_in_dim(slab_scales, first, TOK_DEV, 0).astype(jnp.float32)
            target = (code_rows.reshape(TOK_DEV, COLS // QBLOCK, QBLOCK) * scale_rows[..., None]).reshape(TOK_DEV, COLS)
            errors = (approx - target).astype(jnp.bfloat16)
            grad_attn = jnp.zeros((TOK_DEV, HEADS * HEAD_DIM), jnp.float32)
            for column_block in range(part_count):
                lower = column_block * col_width
                term = jnp.dot(errors[:, lower:lower + col_width], projection[:, lower:lower + col_width].T, preferred_element_type=jnp.float32)
                term_low = lax.optimization_barrier(term.astype(jnp.bfloat16))
                grad_attn = grad_attn + term_low.astype(jnp.float32)
            grad_low = grad_attn.astype(jnp.bfloat16)
            grad_heads = grad_low.reshape(TOK_DEV, KV_HEADS, group_size, HEAD_DIM).transpose(1, 2, 0, 3).astype(jnp.float32)
            row_delta = (grad_heads * attn_wide).sum(-1)
            grad_prob = jnp.einsum('hgqd,hkd->hgqk', grad_heads, value_heads, precision=highest)
            grad_score = (probs * (grad_prob - row_delta[..., None]) * inv_root).astype(jnp.bfloat16).astype(jnp.float32)
            grad_queries = jnp.einsum('hgqk,hkd->hgqd', grad_score, key_heads, precision=highest)
            grad_queries = grad_queries.transpose(2, 0, 1, 3).reshape(TOK_DEV, HEADS * HEAD_DIM).astype(jnp.bfloat16)
            key_piece = jnp.einsum('hgqk,hgqd->hkd', grad_score, queries, precision=highest)
            value_piece = jnp.einsum('hgqk,hgqd->hkd', prob_low.astype(jnp.float32), grad_heads, precision=highest)
            key_low = lax.optimization_barrier(key_piece.astype(jnp.bfloat16))
            value_low = lax.optimization_barrier(value_piece.astype(jnp.bfloat16))
            grad_keys = grad_keys + key_low.astype(jnp.float32)
            grad_values = grad_values + value_low.astype(jnp.float32)
            return ((grad_keys, grad_values), grad_queries)
        zeros_kv = jnp.zeros((KV_HEADS, SEQ_LEN, HEAD_DIM), jnp.float32)
        (grad_keys, grad_values), grad_queries = lax.scan(scan_step, (zeros_kv, zeros_kv), jnp.arange(block_count, dtype=jnp.int32))
        grad_queries = grad_queries.reshape(SEQ_LEN, HEADS * HEAD_DIM)
        grad_keys = grad_keys.transpose(1, 0, 2).reshape(SEQ_LEN, KV_HEADS * HEAD_DIM).astype(jnp.bfloat16)
        grad_values = grad_values.transpose(1, 0, 2).reshape(SEQ_LEN, KV_HEADS * HEAD_DIM).astype(jnp.bfloat16)
        return (grad_queries, grad_keys, grad_values)
    grad_query, grad_key, grad_value = lax.map(one_slab, (query_rows, key_rows, value_rows, teacher_codes, teacher_scales))
    return (grad_query, grad_key, grad_value)
```

```python
import functools
import math

import jax
import jax.numpy as jnp
from jax import lax
from jax.experimental import pallas as pl
from jax.experimental.pallas import tpu as pltpu
from jax.sharding import PartitionSpec as P

HEADS = 16
KV_HEADS = 4
HEAD_DIM = 128
QBLOCK = 128


masked_low = -1e30
QUAD = 4
CHUNKS = 2


def gather_kernel(n_grp, own_ref, all_ref, local_sem, own_sems, z_send, z_recv, x_send, x_recv,
                  y_send, y_recv, d_send, d_recv, r_send, r_recv):
    g = lax.axis_index("grp")
    t = lax.axis_index("tp")
    r = lax.axis_index("rep")
    q = lax.rem(t, QUAD)
    qx = q + 1 - 2 * lax.rem(q, 2)
    qy = lax.rem(q + 2, QUAD)
    qd = lax.rem(qx + 2, QUAD)
    tx = t - q + qx
    ty = t - q + qy
    rows = own_ref.shape[0]
    size = rows // (QUAD * CHUNKS)
    others = n_grp - 1
    to_x, to_y, to_r = {"tp": tx}, {"tp": ty}, {"rep": 1 - r}
    mesh_ids = pl.DeviceIdType.MESH

    barrier = pltpu.get_barrier_semaphore()
    partners = [{"grp": lax.rem(g + k, n_grp)} for k in range(1, n_grp)] + [to_x, to_y, to_r]
    for partner in partners:
        pl.semaphore_signal(barrier, inc=1, device_id=partner, device_id_type=mesh_ids)
    pl.semaphore_wait(barrier, len(partners))

    def spot(quarter, c):
        return pl.ds(pl.multiple_of((quarter * CHUNKS + c) * size, size), size)

    def block(k):
        return lax.rem(g + k, n_grp) * 2 + r

    def sem_at(k, c):
        return c * others + k - 1

    def send(src, dst, sems, index, to):
        return pltpu.make_async_remote_copy(
            src_ref=src, dst_ref=dst, send_sem=sems[0].at[index], recv_sem=sems[1].at[index],
            device_id=to, device_id_type=mesh_ids)

    def forward(k, c, quarter, sems, index, to):
        part = all_ref.at[block(k), spot(quarter, c)]
        return send(part, part, sems, index, to)

    zs, xs, ys, ds, rs = ((z_send, z_recv), (x_send, x_recv), (y_send, y_recv),
                          (d_send, d_recv), (r_send, r_recv))
    started = []

    def go(copy):
        copy.start()
        started.append(copy)

    order = [1, n_grp - 1] + list(range(2, n_grp - 1)) if n_grp > 2 else [1]
    events = [(k, c) for c in range(CHUNKS) for k in order]
    for k, c in events:
        go(send(own_ref.at[spot(q, c)], all_ref.at[block(0), spot(q, c)], zs, sem_at(k, c),
                {"grp": lax.rem(g + n_grp - k, n_grp)}))
    local = pltpu.make_async_copy(own_ref, all_ref.at[block(0)], local_sem.at[0])
    local.start()
    own_swap = pltpu.make_async_remote_copy(
        src_ref=own_ref, dst_ref=all_ref.at[block(0)], send_sem=own_sems.at[0],
        recv_sem=own_sems.at[1], device_id=to_r, device_id_type=mesh_ids)
    own_swap.start()

    swaps = []

    def swap(k, c, quarter, lane):
        copy = forward(k, c, quarter, rs, lane * others * CHUNKS + sem_at(k, c), to_r)
        go(copy)
        swaps.append((k, c, (lane, sem_at(k, c))))

    def on_z(k, c):
        forward(k, c, q, zs, sem_at(k, c), to_x).wait_recv()
        go(forward(k, c, q, xs, sem_at(k, c), to_x))
        go(forward(k, c, q, ys, sem_at(k, c), to_y))
        swap(k, c, q, 0)

    def on_xy(k, c):
        forward(k, c, qx, xs, sem_at(k, c), to_x).wait_recv()
        if c % 2 == 0:
            go(forward(k, c, qx, ds, sem_at(k, c), to_y))
        swap(k, c, qx, 1)
        forward(k, c, qy, ys, sem_at(k, c), to_y).wait_recv()
        if c % 2 == 1:
            go(forward(k, c, qy, ds, sem_at(k, c), to_x))
        swap(k, c, qy, 2)

    def on_d(k, c):
        forward(k, c, qd, ds, sem_at(k, c), to_x).wait_recv()
        swap(k, c, qd, 3)

    lag = 2
    for i in range(len(events) + 2 * lag):
        if i < len(events):
            on_z(*events[i])
        if lag <= i < len(events) + lag:
            on_xy(*events[i - lag])
        if i >= 2 * lag:
            on_d(*events[i - 2 * lag])

    local.wait()
    own_swap.wait_send()
    for copy in started:
        copy.wait_send()
    peer = all_ref.at[lax.rem(g, n_grp) * 2 + 1 - r]
    pltpu.make_async_remote_copy(
        src_ref=own_ref, dst_ref=peer, send_sem=own_sems.at[0],
        recv_sem=own_sems.at[1], device_id=to_r, device_id_type=mesh_ids).wait_recv()
    for lane, quarter in enumerate((q, qx, qy, qd)):
        for k, c in events:
            part = all_ref.at[lax.rem(g + k, n_grp) * 2 + 1 - r, spot(quarter, c)]
            send(part, part, rs, lane * others * CHUNKS + sem_at(k, c), to_r).wait_recv()


def gather_columns(projection, n_grp, n_rep, n_tp):
    rows, width = projection.shape
    if n_rep != 2 or n_grp < 2 or n_tp % QUAD or rows % (QUAD * CHUNKS * 16):
        return lax.all_gather(projection, ("grp", "rep"), axis=0)
    steps = (n_grp - 1) * CHUNKS
    dma = pltpu.SemaphoreType.DMA
    total = n_grp * n_rep * rows * width
    return pl.pallas_call(
        functools.partial(gather_kernel, n_grp),
        out_shape=jax.ShapeDtypeStruct((n_grp * n_rep, rows, width), projection.dtype),
        in_specs=[pl.BlockSpec(memory_space=pltpu.VMEM)],
        out_specs=pl.BlockSpec(memory_space=pltpu.HBM),
        scratch_shapes=[dma((1,)), dma((2,))] + [dma((steps,))] * 8 + [dma((4 * steps,))] * 2,
        compiler_params=pltpu.CompilerParams(collective_id=0, has_side_effects=True),
        cost_estimate=pl.CostEstimate(flops=0, bytes_accessed=12 * total, transcendentals=0),
    )(projection)


def shards(mesh, query_rows, key_rows, value_rows, teacher_codes, teacher_scales, projection):
    rows_dev = query_rows.shape[1]
    group_size = HEADS // KV_HEADS
    inv_root = 1.0 / math.sqrt(HEAD_DIM)
    kv_width = key_rows.shape[2]
    pairs_all = lax.all_gather(
        jnp.concatenate([key_rows, value_rows], 2), ("grp", "rep"), axis=1, tiled=True
    )
    keys_all, values_all = pairs_all[..., :kv_width], pairs_all[..., kv_width:]
    length = keys_all.shape[1]
    key_block = min(1024, length)
    my_index = lax.axis_index(("grp", "rep"))
    first_row = my_index * rows_dev
    needed = (first_row + rows_dev + key_block - 1) // key_block
    queries = query_rows[0].reshape(rows_dev, KV_HEADS, group_size, HEAD_DIM).transpose(1, 2, 0, 3)
    key_heads = keys_all[0].reshape(length, KV_HEADS, HEAD_DIM).transpose(1, 0, 2)
    value_heads = values_all[0].reshape(length, KV_HEADS, HEAD_DIM).transpose(1, 0, 2)
    row_pos = first_row + jnp.arange(rows_dev, dtype=jnp.int32)
    slab_codes, slab_scales = (
        lax.all_to_all(teacher_codes, "tp", split_axis=0, concat_axis=2, tiled=True),
        lax.all_to_all(teacher_scales, "tp", split_axis=0, concat_axis=2, tiled=True),
    )

    def block_scores(block_index):
        offset = block_index * key_block
        raw_scores = (
            jnp.einsum("hgqd,hkd->hgqk", queries, key_heads, preferred_element_type=jnp.float32)
            * inv_root
        )
        col_pos = offset + jnp.arange(key_block, dtype=jnp.int32)
        allowed = col_pos[None, :] <= row_pos[:, None]
        return (jnp.where(allowed, raw_scores, masked_low), key_heads, value_heads)

    def stats_step(block_index, running):
        row_peak, row_total = running
        scores, key_part, value_part = block_scores(block_index)
        new_peak = jnp.maximum(row_peak, scores.max(-1))
        row_total = row_total * jnp.exp(row_peak - new_peak) + jnp.exp(
            scores - new_peak[..., None]
        ).sum(-1)
        return (new_peak, row_total)

    stat_shape = (KV_HEADS, group_size, rows_dev)
    row_peak, row_total = lax.fori_loop(
        0,
        needed,
        stats_step,
        (jnp.full(stat_shape, masked_low, jnp.float32), jnp.zeros(stat_shape, jnp.float32)),
    )

    def block_probs(scores):
        return jnp.exp(scores - row_peak[..., None]) / row_total[..., None]

    def output_step(block_index, running):
        scores, key_part, value_part = block_scores(block_index)
        prob_low = block_probs(scores).astype(jnp.bfloat16)
        return running + jnp.einsum(
            "hgqk,hkd->hgqd", prob_low, value_part, preferred_element_type=jnp.float32
        )

    attn_wide = lax.fori_loop(
        0, needed, output_step, jnp.zeros((KV_HEADS, group_size, rows_dev, HEAD_DIM), jnp.float32)
    )
    attn_low = (
        attn_wide.transpose(2, 0, 1, 3).reshape(rows_dev, HEADS * HEAD_DIM).astype(jnp.bfloat16)
    )
    col_width = projection.shape[1]
    shaped = gather_columns(
        projection, mesh.shape["grp"], mesh.shape["rep"], mesh.shape["tp"]
    )
    pieces = shaped.shape[0]
    approx = jnp.einsum("td,sdc->tsc", attn_low, shaped, preferred_element_type=jnp.float32)
    code_rows = slab_codes[0].astype(jnp.float32)
    scale_rows = slab_scales[0].astype(jnp.float32)
    target = (code_rows.reshape(rows_dev, -1, QBLOCK) * scale_rows[..., None]).reshape(
        rows_dev, pieces, col_width
    )
    errors = (approx - target).astype(jnp.bfloat16)
    partial_terms = jnp.einsum(
        "tsc,sdc->std", errors, shaped, preferred_element_type=jnp.float32
    ).astype(jnp.bfloat16)
    grad_attn = partial_terms.astype(jnp.float32).sum(0)
    grad_low = grad_attn.astype(jnp.bfloat16)
    grad_heads = grad_low.reshape(rows_dev, KV_HEADS, group_size, HEAD_DIM).transpose(1, 2, 0, 3)
    row_delta = (grad_heads.astype(jnp.float32) * attn_wide).sum(-1)

    def back_step(block_index, running):
        grad_queries, grad_keys, grad_values = running
        scores, key_part, value_part = block_scores(block_index)
        probs = block_probs(scores)
        prob_low = probs.astype(jnp.bfloat16)
        grad_prob = jnp.einsum(
            "hgqd,hkd->hgqk", grad_heads, value_part, preferred_element_type=jnp.float32
        )
        grad_score = (probs * (grad_prob - row_delta[..., None]) * inv_root).astype(jnp.bfloat16)
        grad_queries = grad_queries + jnp.einsum(
            "hgqk,hkd->hgqd", grad_score, key_part, preferred_element_type=jnp.float32
        )
        key_piece = jnp.einsum(
            "hgqk,hgqd->hkd", grad_score, queries, preferred_element_type=jnp.float32
        )
        value_piece = jnp.einsum(
            "hgqk,hgqd->hkd", prob_low, grad_heads, preferred_element_type=jnp.float32
        )
        grad_keys = key_piece
        grad_values = value_piece
        return (grad_queries, grad_keys, grad_values)

    zeros_kv = jnp.zeros((KV_HEADS, length, HEAD_DIM), jnp.float32)
    grad_queries, grad_keys, grad_values = lax.fori_loop(
        0,
        needed,
        back_step,
        (jnp.zeros((KV_HEADS, group_size, rows_dev, HEAD_DIM), jnp.float32), zeros_kv, zeros_kv),
    )
    key_terms = grad_keys.transpose(1, 0, 2).reshape(1, length, KV_HEADS * HEAD_DIM)
    value_terms = grad_values.transpose(1, 0, 2).reshape(1, length, KV_HEADS * HEAD_DIM)
    pair_terms = jnp.concatenate([key_terms, value_terms], 2).astype(jnp.bfloat16)
    pair_grad = lax.psum_scatter(
        pair_terms, ("grp", "rep"), scatter_dimension=1, tiled=True
    )
    key_grad, value_grad = pair_grad[..., :kv_width], pair_grad[..., kv_width:]
    query_grad = (
        grad_queries.transpose(2, 0, 1, 3)
        .reshape(1, rows_dev, HEADS * HEAD_DIM)
        .astype(jnp.bfloat16)
    )
    return (query_grad, key_grad.astype(jnp.bfloat16), value_grad.astype(jnp.bfloat16))


def solution(mesh):
    placed = (
        P("tp", ("grp", "rep"), None),
        P("tp", ("grp", "rep"), None),
        P("tp", ("grp", "rep"), None),
        P(None, ("grp", "rep"), "tp"),
        P(None, ("grp", "rep"), "tp"),
        P(None, ("grp", "rep")),
    )
    return jax.shard_map(
        functools.partial(shards, mesh),
        mesh=mesh,
        in_specs=placed,
        out_specs=(
            P("tp", ("grp", "rep"), None),
            P("tp", ("grp", "rep"), None),
            P("tp", ("grp", "rep"), None),
        ),
        check_vma=False,
    )
```

```python
import functools
import math

import jax
import jax.numpy as jnp
from jax import lax
from jax.experimental import pallas as pl
from jax.experimental.pallas import tpu as pltpu
from jax.sharding import PartitionSpec as P

HEADS = 16
KV_HEADS = 4
HEAD_DIM = 128
QBLOCK = 128


masked_low = -1e30
QUAD = 4
CHUNKS = 2


def gather_kernel(n_grp, own_ref, all_ref, local_sem, own_sems, z_send, z_recv, x_send, x_recv,
                  y_send, y_recv, d_send, d_recv, r_send, r_recv):
    g = lax.axis_index("grp")
    t = lax.axis_index("tp")
    r = lax.axis_index("rep")
    q = lax.rem(t, QUAD)
    qx = q + 1 - 2 * lax.rem(q, 2)
    qy = lax.rem(q + 2, QUAD)
    qd = lax.rem(qx + 2, QUAD)
    tx = t - q + qx
    ty = t - q + qy
    rows = own_ref.shape[0]
    size = rows // (QUAD * CHUNKS)
    others = n_grp - 1
    to_x, to_y, to_r = {"tp": tx}, {"tp": ty}, {"rep": 1 - r}
    mesh_ids = pl.DeviceIdType.MESH

    barrier = pltpu.get_barrier_semaphore()
    partners = [{"grp": lax.rem(g + k, n_grp)} for k in range(1, n_grp)] + [to_x, to_y, to_r]
    for partner in partners:
        pl.semaphore_signal(barrier, inc=1, device_id=partner, device_id_type=mesh_ids)
    pl.semaphore_wait(barrier, len(partners))

    def spot(quarter, c):
        return pl.ds(pl.multiple_of((quarter * CHUNKS + c) * size, size), size)

    def block(k):
        return lax.rem(g + k, n_grp) * 2 + r

    def sem_at(k, c):
        return c * others + k - 1

    def send(src, dst, sems, index, to):
        return pltpu.make_async_remote_copy(
            src_ref=src, dst_ref=dst, send_sem=sems[0].at[index], recv_sem=sems[1].at[index],
            device_id=to, device_id_type=mesh_ids)

    def forward(k, c, quarter, sems, index, to):
        part = all_ref.at[block(k), spot(quarter, c)]
        return send(part, part, sems, index, to)

    zs, xs, ys, ds, rs = ((z_send, z_recv), (x_send, x_recv), (y_send, y_recv),
                          (d_send, d_recv), (r_send, r_recv))
    started = []

    def go(copy):
        copy.start()
        started.append(copy)

    order = [1, n_grp - 1] + list(range(2, n_grp - 1)) if n_grp > 2 else [1]
    events = [(k, c) for c in range(CHUNKS) for k in order]
    for k, c in events:
        go(send(own_ref.at[spot(q, c)], all_ref.at[block(0), spot(q, c)], zs, sem_at(k, c),
                {"grp": lax.rem(g + n_grp - k, n_grp)}))
    local = pltpu.make_async_copy(own_ref, all_ref.at[block(0)], local_sem.at[0])
    local.start()
    own_swap = pltpu.make_async_remote_copy(
        src_ref=own_ref, dst_ref=all_ref.at[block(0)], send_sem=own_sems.at[0],
        recv_sem=own_sems.at[1], device_id=to_r, device_id_type=mesh_ids)
    own_swap.start()

    swaps = []

    def swap(k, c, quarter, lane):
        copy = forward(k, c, quarter, rs, lane * others * CHUNKS + sem_at(k, c), to_r)
        go(copy)
        swaps.append((k, c, (lane, sem_at(k, c))))

    def on_z(k, c):
        forward(k, c, q, zs, sem_at(k, c), to_x).wait_recv()
        go(forward(k, c, q, xs, sem_at(k, c), to_x))
        go(forward(k, c, q, ys, sem_at(k, c), to_y))
        swap(k, c, q, 0)

    def on_xy(k, c):
        forward(k, c, qx, xs, sem_at(k, c), to_x).wait_recv()
        if events.index((k, c)) % 2 == 0:
            go(forward(k, c, qx, ds, sem_at(k, c), to_y))
        swap(k, c, qx, 1)
        forward(k, c, qy, ys, sem_at(k, c), to_y).wait_recv()
        if events.index((k, c)) % 2 == 1:
            go(forward(k, c, qy, ds, sem_at(k, c), to_x))
        swap(k, c, qy, 2)

    def on_d(k, c):
        forward(k, c, qd, ds, sem_at(k, c), to_x).wait_recv()
        swap(k, c, qd, 3)

    lag = 2
    for i in range(len(events) + 2 * lag):
        if i < len(events):
            on_z(*events[i])
        if lag <= i < len(events) + lag:
            on_xy(*events[i - lag])
        if i >= 2 * lag:
            on_d(*events[i - 2 * lag])

    local.wait()
    own_swap.wait_send()
    for copy in started:
        copy.wait_send()
    peer = all_ref.at[lax.rem(g, n_grp) * 2 + 1 - r]
    pltpu.make_async_remote_copy(
        src_ref=own_ref, dst_ref=peer, send_sem=own_sems.at[0],
        recv_sem=own_sems.at[1], device_id=to_r, device_id_type=mesh_ids).wait_recv()
    for lane, quarter in enumerate((q, qx, qy, qd)):
        for k, c in events:
            part = all_ref.at[lax.rem(g + k, n_grp) * 2 + 1 - r, spot(quarter, c)]
            send(part, part, rs, lane * others * CHUNKS + sem_at(k, c), to_r).wait_recv()


def gather_columns(projection, n_grp, n_rep, n_tp):
    rows, width = projection.shape
    if n_rep != 2 or n_grp < 2 or n_tp % QUAD or rows % (QUAD * CHUNKS * 16):
        return lax.all_gather(projection, ("grp", "rep"), axis=0)
    steps = (n_grp - 1) * CHUNKS
    dma = pltpu.SemaphoreType.DMA
    total = n_grp * n_rep * rows * width
    return pl.pallas_call(
        functools.partial(gather_kernel, n_grp),
        out_shape=jax.ShapeDtypeStruct((n_grp * n_rep, rows, width), projection.dtype),
        in_specs=[pl.BlockSpec(memory_space=pltpu.VMEM)],
        out_specs=pl.BlockSpec(memory_space=pltpu.HBM),
        scratch_shapes=[dma((1,)), dma((2,))] + [dma((steps,))] * 8 + [dma((4 * steps,))] * 2,
        compiler_params=pltpu.CompilerParams(collective_id=0, has_side_effects=True),
        cost_estimate=pl.CostEstimate(flops=0, bytes_accessed=12 * total, transcendentals=0),
    )(projection)


def shards(mesh, query_rows, key_rows, value_rows, teacher_codes, teacher_scales, projection):
    rows_dev = query_rows.shape[1]
    group_size = HEADS // KV_HEADS
    inv_root = 1.0 / math.sqrt(HEAD_DIM)
    kv_width = key_rows.shape[2]
    pairs_all = lax.all_gather(
        jnp.concatenate([key_rows, value_rows], 2), ("grp", "rep"), axis=1, tiled=True
    )
    keys_all, values_all = pairs_all[..., :kv_width], pairs_all[..., kv_width:]
    length = keys_all.shape[1]
    my_index = lax.axis_index(("grp", "rep"))
    first_row = my_index * rows_dev
    queries = query_rows[0].reshape(rows_dev, KV_HEADS, group_size, HEAD_DIM).transpose(1, 2, 0, 3)
    key_heads = keys_all[0].reshape(length, KV_HEADS, HEAD_DIM).transpose(1, 0, 2)
    value_heads = values_all[0].reshape(length, KV_HEADS, HEAD_DIM).transpose(1, 0, 2)
    row_pos = first_row + jnp.arange(rows_dev, dtype=jnp.int32)
    slab_codes, slab_scales = (
        lax.all_to_all(teacher_codes, "tp", split_axis=0, concat_axis=2, tiled=True),
        lax.all_to_all(teacher_scales, "tp", split_axis=0, concat_axis=2, tiled=True),
    )

    raw_scores = (
        jnp.einsum("hgqd,hkd->hgqk", queries, key_heads, preferred_element_type=jnp.float32)
        * inv_root
    )
    allowed = jnp.arange(length, dtype=jnp.int32)[None, :] <= row_pos[:, None]
    scores = jnp.where(allowed, raw_scores, masked_low)
    row_peak = scores.max(-1, keepdims=True)
    shifted = jnp.exp(scores - row_peak)
    probs = shifted / shifted.sum(-1, keepdims=True)
    prob_low = probs.astype(jnp.bfloat16)
    attn_wide = jnp.einsum(
        "hgqk,hkd->hgqd", prob_low, value_heads, preferred_element_type=jnp.float32
    )
    attn_low = (
        attn_wide.transpose(2, 0, 1, 3).reshape(rows_dev, HEADS * HEAD_DIM).astype(jnp.bfloat16)
    )
    col_width = projection.shape[1]
    shaped = gather_columns(
        projection, mesh.shape["grp"], mesh.shape["rep"], mesh.shape["tp"]
    )
    pieces = shaped.shape[0]
    approx = jnp.einsum("td,sdc->tsc", attn_low, shaped, preferred_element_type=jnp.float32)
    code_rows = slab_codes[0].astype(jnp.float32)
    scale_rows = slab_scales[0].astype(jnp.float32)
    target = (code_rows.reshape(rows_dev, -1, QBLOCK) * scale_rows[..., None]).reshape(
        rows_dev, pieces, col_width
    )
    errors = (approx - target).astype(jnp.bfloat16)
    partial_terms = jnp.einsum(
        "tsc,sdc->std", errors, shaped, preferred_element_type=jnp.float32
    ).astype(jnp.bfloat16)
    grad_attn = partial_terms.astype(jnp.float32).sum(0)
    grad_low = grad_attn.astype(jnp.bfloat16)
    grad_heads = grad_low.reshape(rows_dev, KV_HEADS, group_size, HEAD_DIM).transpose(1, 2, 0, 3)
    row_delta = (grad_heads.astype(jnp.float32) * attn_wide).sum(-1)

    grad_values = jnp.einsum(
        "hgqk,hgqd->hkd", prob_low, grad_heads, preferred_element_type=jnp.float32
    )
    grad_prob = jnp.einsum(
        "hgqd,hkd->hgqk", grad_heads, value_heads, preferred_element_type=jnp.float32
    )
    grad_score = (probs * (grad_prob - row_delta[..., None]) * inv_root).astype(jnp.bfloat16)
    grad_queries = jnp.einsum(
        "hgqk,hkd->hgqd", grad_score, key_heads, preferred_element_type=jnp.float32
    )
    grad_keys = jnp.einsum(
        "hgqk,hgqd->hkd", grad_score, queries, preferred_element_type=jnp.float32
    )
    key_terms = grad_keys.transpose(1, 0, 2).reshape(1, length, KV_HEADS * HEAD_DIM)
    value_terms = grad_values.transpose(1, 0, 2).reshape(1, length, KV_HEADS * HEAD_DIM)
    pair_terms = jnp.concatenate([key_terms, value_terms], 2).astype(jnp.bfloat16)
    pair_grad = lax.psum_scatter(
        pair_terms, ("grp", "rep"), scatter_dimension=1, tiled=True
    )
    key_grad, value_grad = pair_grad[..., :kv_width], pair_grad[..., kv_width:]
    query_grad = (
        grad_queries.transpose(2, 0, 1, 3)
        .reshape(1, rows_dev, HEADS * HEAD_DIM)
        .astype(jnp.bfloat16)
    )
    return (query_grad, key_grad.astype(jnp.bfloat16), value_grad.astype(jnp.bfloat16))


def solution(mesh):
    placed = (
        P("tp", ("grp", "rep"), None),
        P("tp", ("grp", "rep"), None),
        P("tp", ("grp", "rep"), None),
        P(None, ("grp", "rep"), "tp"),
        P(None, ("grp", "rep"), "tp"),
        P(None, ("grp", "rep")),
    )
    return jax.shard_map(
        functools.partial(shards, mesh),
        mesh=mesh,
        in_specs=placed,
        out_specs=(
            P("tp", ("grp", "rep"), None),
            P("tp", ("grp", "rep"), None),
            P("tp", ("grp", "rep"), None),
        ),
        check_vma=False,
    )
```
